32 devices in a mesh: node: 4 (over z), local: 8 (over y, x, core).
Axes of the slice: x: 2, y: 2, z: 4, core: 2. Of those that a mesh axis runs over, the one named last changes fastest.
Arguments:
- tokens: bfloat16 [512, 7168], P(('node', 'local')), may hold values from -6 to 6
- grad_out: bfloat16 [512, 7168], P(('node', 'local')), may hold values from -6 to 6
- gates: bfloat16 [512, 3], P(('node', 'local')), may hold values from 0.19921875 to 1
- expert_ids: int32 [512, 3], P(('node', 'local')), may hold values from 0 to 7, as said below
- w_gate: bfloat16 [4, 7168, 2048], P('node', None, 'local'), may hold values from -0.0625 to 0.0625
- w_up: bfloat16 [4, 7168, 2048], P('node', None, 'local'), may hold values from -0.0625 to 0.0625
- w_down: bfloat16 [4, 7168, 2048], P('node', None, 'local'), may hold values from -0.1875 to 0.1875
- s_gate: bfloat16 [7168, 2048], P(None, 'local'), may hold values from -0.0625 to 0.0625
- s_up: bfloat16 [7168, 2048], P(None, 'local'), may hold values from -0.0625 to 0.0625
- s_down: bfloat16 [7168, 2048], P(None, 'local'), may hold values from -0.125 to 0.125
Outputs:
- dx: bfloat16 [512, 7168], P(('node', 'local'))
- dgates: float32 [512, 3], P(('node', 'local'))
- d_w_gate: bfloat16 [4, 7168, 2048], P('node', None, 'local')
- d_w_up: bfloat16 [4, 7168, 2048], P('node', None, 'local')
- d_w_down: bfloat16 [4, 7168, 2048], P('node', None, 'local')
- d_s_gate: bfloat16 [7168, 2048], P('node', 'local')
- d_s_up: bfloat16 [7168, 2048], P('node', 'local')
- d_s_down: bfloat16 [7168, 2048], P('node', 'local')
The draws below stay inside these ranges and needn't reach their ends.
Inputs may be any that keep to these rules, and one draw needn't show every extreme that they name: `expert_ids`: each token names both experts of one node and one expert of a second node. Of the tokens of one device exactly 8 name experts of each node and at most 8 name any one expert; for every node one of its experts is named by exactly 8 tokens of every device.
All inputs are finite; a program needn't handle non-finite values.
Results may differ from the reference program's by a relative error of at most 0.014.
Values may be sent and summed in bfloat16 or wider, within the bound.
A program may use at most 192 MiB of HBM per device.

```python
import jax
import jax.numpy as jnp
from jax import lax

D = 7168
FF = 1024
FFS = 2048
TOPK = 3
E_NODE = 2
TOK_DEV = 16
TOKENS = 512
EXPERTS = 8
N_NODE = 4
N_LOCAL = 8


def draw_expert_ids(key, part):
    node_count = EXPERTS // E_NODE
    device_count = TOKENS // TOK_DEV
    keys = jax.random.split(key, 4)
    node_order = jax.vmap(lambda item: jax.random.permutation(item, node_count))(jax.random.split(keys[0], device_count))
    position = jnp.arange(TOK_DEV, dtype=jnp.int32)
    first_slot = position % node_count
    second_slot = (first_slot + 1 + position // node_count % (node_count - 1)) % node_count
    first = jnp.take(node_order, first_slot, axis=1)
    second = jnp.take(node_order, second_slot, axis=1)
    busy = jax.random.randint(keys[1], (node_count,), 0, E_NODE)
    single = jnp.take(busy, second)
    trio = jnp.stack([first * E_NODE, first * E_NODE + 1, second * E_NODE + single], axis=-1)
    shift = jax.random.randint(keys[2], (device_count, TOK_DEV, 1), 0, 3)
    column = (jnp.arange(3, dtype=jnp.int32)[None, None, :] + shift) % 3
    trio = jnp.take_along_axis(trio, column, axis=2)
    shuffle = jax.vmap(lambda item: jax.random.permutation(item, TOK_DEV))(jax.random.split(keys[3], device_count))
    trio = jnp.take_along_axis(trio, shuffle[:, :, None], axis=1)
    return trio.reshape(TOKENS, 3).astype(jnp.int32)


def shard_levels(stream_key, extent, shards, least, top_value):
    loudness, own = 1.0, jax.random.fold_in(stream_key, 6)
    for dim, blocks in shards:
        heights = jnp.exp(jax.random.uniform(jax.random.fold_in(own, dim), (blocks,), jnp.float32, least / len(shards), top_value / len(shards)))
        loudness = loudness * jnp.repeat(heights, extent[dim] // blocks).reshape([-1 if axis == dim else 1 for axis in range(len(extent))])
    return loudness


def bell_draw(own_key, extent, deviation, bound, shards=(), kind=jnp.bfloat16):
    factor_of = shard_levels(own_key, extent, shards, -0.22, 0.18) if shards else 1.0
    array = jax.random.normal(own_key, extent, jnp.float32) * deviation * factor_of
    return jnp.minimum(jnp.maximum(array, -bound), bound).astype(kind)


def setup_inputs(seed: int = 0) -> dict:
    key_of = jax.random.split(jax.random.key(seed), 11)
    tokens = bell_draw(key_of[0], (TOKENS, D), 1.0, 6.0, ((0, 32),))
    grad_out = bell_draw(key_of[1], (TOKENS, D), 1.0, 6.0, ((0, 32),))
    gates = jnp.clip(0.19921875 + 0.80078125 * jax.random.uniform(key_of[2], (TOKENS, TOPK), jnp.float32) ** shard_levels(key_of[2], (TOKENS, TOPK), ((0, 32),), -0.2, 0.2), 0.19921875, 1.0).astype(jnp.bfloat16)
    expert_ids = draw_expert_ids(jax.random.fold_in(key_of[10], 71), 0)
    w_gate = bell_draw(key_of[4], (N_NODE, D, E_NODE * FF), D ** -0.5, 0.0625, ((0, 4), (2, 8)))
    w_up = bell_draw(key_of[5], (N_NODE, D, E_NODE * FF), D ** -0.5, 0.0625, ((0, 4), (2, 8)))
    w_down = bell_draw(key_of[6], (N_NODE, D, E_NODE * FF), FF ** -0.5, 0.1875, ((0, 4), (2, 8)))
    s_gate = bell_draw(key_of[7], (D, FFS), D ** -0.5, 0.0625, ((1, 8),))
    s_up = bell_draw(key_of[8], (D, FFS), D ** -0.5, 0.0625, ((1, 8),))
    s_down = bell_draw(key_of[9], (D, FFS), FFS ** -0.5, 0.125, ((1, 8),))
    return {"tokens": tokens, "grad_out": grad_out, "gates": gates, "expert_ids": expert_ids, "w_gate": w_gate, "w_up": w_up, "w_down": w_down, "s_gate": s_gate, "s_up": s_up, "s_down": s_down}


def silu_parts(pre_gate):
    sig = jax.nn.sigmoid(pre_gate)
    return pre_gate * sig, sig * (1.0 + pre_gate * (1.0 - sig))


def contract_first(left, right):
    return lax.dot_general(left, right, (((0,), (0,)), ((), ())), preferred_element_type=jnp.float32)


def contract_last(left, right):
    return lax.dot_general(left, right, (((1,), (1,)), ((), ())), preferred_element_type=jnp.float32)


def ffn_backward(rows_in, rows_grad, weight, gate_w, up_w, down_w):
    pre_gate = jnp.dot(rows_in, gate_w, preferred_element_type=jnp.float32)
    pre_up = jnp.dot(rows_in, up_w, preferred_element_type=jnp.float32)
    activ, slope = silu_parts(pre_gate)
    hidden = activ * pre_up
    upstream = jnp.dot(rows_grad, down_w, preferred_element_type=jnp.float32)
    scaled = weight * upstream
    grad_up = (scaled * activ).astype(jnp.bfloat16)
    grad_gate = (scaled * pre_up * slope).astype(jnp.bfloat16)
    weighted = (weight * hidden).astype(jnp.bfloat16)
    return grad_gate, grad_up, weighted, hidden * upstream


def block_rows(grad_gate, grad_up, gate_w, up_w, width):
    blocks = gate_w.shape[1] // width

    def step(index, total):
        start = index * width
        part = contract_last(lax.dynamic_slice_in_dim(grad_gate, start, width, 1), lax.dynamic_slice_in_dim(gate_w, start, width, 1))
        part = part + contract_last(lax.dynamic_slice_in_dim(grad_up, start, width, 1), lax.dynamic_slice_in_dim(up_w, start, width, 1))
        rounded = lax.optimization_barrier(part.astype(jnp.bfloat16))
        return total + rounded.astype(jnp.float32)

    return lax.fori_loop(0, blocks, step, jnp.zeros((grad_gate.shape[0], gate_w.shape[0]), jnp.float32))


def block_stat(product, width):
    sums = jnp.sum(product.reshape(product.shape[0], -1, width), axis=2)
    return jnp.sum(lax.optimization_barrier(sums.astype(jnp.bfloat16)).astype(jnp.float32), axis=1)


def reference(tokens, grad_out, gates, expert_ids, w_gate, w_up, w_down, s_gate, s_up, s_down):
    n_tok = tokens.shape[0]
    width = tokens.shape[1]
    device_count = n_tok // TOK_DEV
    slots = device_count * (2 * TOK_DEV // N_NODE)
    group_size = N_LOCAL // E_NODE
    ff_block = FF // group_size
    gate_all = gates.astype(jnp.float32)
    positions = jnp.arange(n_tok, dtype=jnp.int32)

    def per_expert(carry, expert):
        dx_acc, dgate_acc = carry
        chosen = expert_ids == expert
        member = jnp.any(chosen, axis=1)
        weight = jnp.sum(jnp.where(chosen, gate_all, 0.0), axis=1)
        ranking = jnp.cumsum(member.astype(jnp.int32)) - 1
        target = jnp.where(member, ranking, slots).astype(jnp.int32)
        index = jnp.zeros((slots + 1,), jnp.int32).at[target].set(positions)[:slots]
        valid = jnp.zeros((slots + 1,), jnp.float32).at[target].set(1.0)[:slots]
        rows_in = tokens[index]
        rows_grad = grad_out[index]
        row_weight = (weight[index] * valid)[:, None]
        node = expert // E_NODE
        column = (expert % E_NODE) * FF
        gate_w = lax.dynamic_slice_in_dim(lax.dynamic_index_in_dim(w_gate, node, 0, keepdims=False), column, FF, 1)
        up_w = lax.dynamic_slice_in_dim(lax.dynamic_index_in_dim(w_up, node, 0, keepdims=False), column, FF, 1)
        down_w = lax.dynamic_slice_in_dim(lax.dynamic_index_in_dim(w_down, node, 0, keepdims=False), column, FF, 1)
        grad_gate, grad_up, weighted, product = ffn_backward(rows_in, rows_grad, row_weight, gate_w, up_w, down_w)
        partial_value = block_rows(grad_gate, grad_up, gate_w, up_w, ff_block)
        stat = block_stat(product, ff_block)
        dx_acc = dx_acc.at[index].add(partial_value * valid[:, None])
        token_stat = jnp.zeros((n_tok,), jnp.float32).at[index].add(stat * valid)
        dgate_acc = dgate_acc + jnp.where(chosen, token_stat[:, None], 0.0)
        grads = (contract_first(rows_in, grad_gate).astype(jnp.bfloat16), contract_first(rows_in, grad_up).astype(jnp.bfloat16), contract_first(rows_grad, weighted).astype(jnp.bfloat16))
        return (dx_acc, dgate_acc), grads

    start_carry = (jnp.zeros((n_tok, width), jnp.float32), jnp.zeros(expert_ids.shape, jnp.float32))
    (dx_routed, dgates), stacked = lax.scan(per_expert, start_carry, jnp.arange(E_NODE * N_NODE, dtype=jnp.int32))

    def arrange(grad):
        shaped = grad.reshape(N_NODE, E_NODE, width, FF)
        return jnp.transpose(shaped, (0, 2, 1, 3)).reshape(N_NODE, width, E_NODE * FF)

    unit_weight = jnp.ones((n_tok, 1), jnp.float32)
    grad_gate, grad_up, weighted, product = ffn_backward(tokens, grad_out, unit_weight, s_gate, s_up, s_down)
    dx_shared = block_rows(grad_gate, grad_up, s_gate, s_up, FFS // N_LOCAL)
    per_node = n_tok // N_NODE

    def node_step(index, totals):
        start = index * per_node
        rows_in = lax.dynamic_slice_in_dim(tokens, start, per_node, 0)
        rows_grad = lax.dynamic_slice_in_dim(grad_out, start, per_node, 0)
        parts = (contract_first(rows_in, lax.dynamic_slice_in_dim(grad_gate, start, per_node, 0)), contract_first(rows_in, lax.dynamic_slice_in_dim(grad_up, start, per_node, 0)), contract_first(rows_grad, lax.dynamic_slice_in_dim(weighted, start, per_node, 0)))
        return tuple(total + lax.optimization_barrier(part.astype(jnp.bfloat16)).astype(jnp.float32) for total, part in zip(totals, parts))

    empty = jnp.zeros((width, FFS), jnp.float32)
    shared = lax.fori_loop(0, N_NODE, node_step, (empty, empty, empty))
    dx = (dx_routed + dx_shared).astype(jnp.bfloat16)
    return (dx, dgates, arrange(stacked[0]), arrange(stacked[1]), arrange(stacked[2]), shared[0].astype(jnp.bfloat16), shared[1].astype(jnp.bfloat16), shared[2].astype(jnp.bfloat16))
```

```python
import functools

import jax
import jax.numpy as jnp
from jax import lax
from jax.experimental import pallas as pl
from jax.experimental.pallas import tpu as pltpu
from jax.sharding import PartitionSpec as P

E_NODE = 2
LANES = 128
PERM = 64
MESH = pl.DeviceIdType.MESH
GROUPS = 2
BF16, F32, I32 = jnp.bfloat16, jnp.float32, jnp.int32


def masks_of(local_count):
    bits = local_count.bit_length() - 1
    return [1 << b for b in range(1, bits)] + [1]


def near_first(node_count):
    return sorted(range(1, node_count), key=lambda s: min(s, node_count - s))


def dot(left, right):
    return jnp.dot(left, right, preferred_element_type=F32)


def contract_first(left, right):
    return lax.dot_general(left, right, (((0,), (0,)), ((), ())), preferred_element_type=F32)


def contract_last(left, right):
    return lax.dot_general(left, right, (((1,), (1,)), ((), ())), preferred_element_type=F32)


def iota(shape, axis):
    return lax.broadcasted_iota(I32, shape, axis)


def flag(values):
    return jnp.where(values, 1.0, 0.0).astype(F32)


def routing_plan(ids, gates, n, nodes, cap):
    held = ids.shape[0]
    shift = cap.bit_length() - 1
    rest = held - cap
    rows, rest_rows = nodes * cap, nodes * rest
    half = cap // 2
    eye = flag(iota((held, held), 0) == iota((held, held), 1))
    ids_t = contract_first(ids.astype(F32), eye).astype(I32)
    gates_t = contract_first(gates.astype(F32), eye)
    node = ids_t >> 1
    which = ids_t & 1
    rel = node - n
    rel = jnp.where(rel < 0, rel + nodes, rel)
    count = ids.shape[1]
    lane_node = iota((nodes, held), 0)
    hit = jnp.zeros((nodes, held), F32)
    gate_of = [jnp.zeros((nodes, held), F32) for _ in range(E_NODE)]
    for k in range(count):
        here = lane_node == rel[k : k + 1, :]
        hit = jnp.maximum(hit, flag(here))
        for e in range(E_NODE):
            named = here & (which[k : k + 1, :] == e)
            gate_of[e] = gate_of[e] + jnp.where(named, gates_t[k : k + 1, :], 0.0)
    upper = flag(iota((held, held), 0) <= iota((held, held), 1))
    rank = dot(hit, upper) - 1.0
    spread = flag((iota((rows, nodes), 0) >> shift) == iota((rows, nodes), 1))
    slot = (iota((rows, held), 0) & (cap - 1)).astype(F32)
    first = flag((dot(spread, hit) > 0.5) & (dot(spread, rank) == slot))

    row, lane = iota((rows, rows), 0), iota((rows, rows), 1)
    unit = flag(row == lane)
    ends = contract_last(first, first) * (1.0 - unit)
    pairs = flag((row ^ 1) == lane)
    reach = unit + dot(ends, pairs)
    for _ in range((held - 1).bit_length()):
        reach = jnp.minimum(dot(reach, reach), 1.0)
    number = lane.astype(F32)
    far = dot(ends, reach)
    label = jnp.min(jnp.where(reach > 0.5, number, float(rows)), axis=1, keepdims=True)
    other = jnp.min(jnp.where(far > 0.5, number, float(rows)), axis=1, keepdims=True)
    taken = flag(label < other)
    same = (row >> shift) == (lane >> shift)
    before = flag(same & (lane < row))
    taken_wide = jnp.broadcast_to(taken, (rows, LANES))
    taken_rank = dot(before, taken_wide)[:, 0:1]
    left_rank = dot(before, 1.0 - taken_wide)[:, 0:1]
    place = jnp.where(taken > 0.5, taken_rank, left_rank + float(half))
    move = flag(same & (place == (lane & (cap - 1)).astype(F32)))
    pick = contract_first(move, first)

    assigned = pick * flag((iota((rows, held), 0) & (cap - 1)) < half)
    weights = [
        jnp.sum(pick * dot(spread, gate_of[e]), axis=1, keepdims=True) for e in range(E_NODE)
    ]
    spot = flag(iota((rows, LANES), 1) == iota((rows, LANES), 0) + PERM)
    lanes = iota((rows, LANES), 1)
    meta = dot(contract_last(pick, assigned), spot)
    for e in range(E_NODE):
        meta = meta + jnp.where(lanes == e, weights[e], 0.0)

    shape = (rest_rows, held)
    block = jnp.zeros(shape, I32)
    for r in range(1, nodes):
        block = block + jnp.where(iota(shape, 0) >= r * rest, 1, 0)
    within = (iota(shape, 0) - block * rest).astype(F32)
    spread_rest = flag(block[:, 0:1] == iota((rest_rows, nodes), 1))
    away = 1.0 - hit
    away_rank = dot(away, upper) - 1.0
    absent = flag((dot(spread_rest, away) > 0.5) & (dot(spread_rest, away_rank) == within))
    meta_rest = dot(contract_last(absent, assigned), spot)
    return pick, meta, absent, meta_rest


def silu_parts(pre_gate):
    sig = jax.nn.sigmoid(pre_gate)
    return (pre_gate * sig, sig * (1.0 + pre_gate * (1.0 - sig)))


def ffn_backward(pre_gate, pre_up, upstream, weight):
    activ, slope = silu_parts(pre_gate)
    hidden = activ * pre_up
    scaled = weight * upstream
    grad_up = (scaled * activ).astype(BF16)
    grad_gate = (scaled * pre_up * slope).astype(BF16)
    weighted = (weight * hidden).astype(BF16)
    return (grad_gate, grad_up, weighted, hidden * upstream)


def main_kernel(
    nodes, local_count, cap,
    tok, grad, ids, gates, w0, w1, w2, w3, w4, w5,
    rows_out, grads_out, packs, ext, back, pick_out,
    rows, away, mine, wbuf, part, land, pre, packed,
    send_sem, recv_sem, copy_sem,
):
    n, l = lax.axis_index("node"), lax.axis_index("local")
    held, width = tok.shape
    units = w0.shape[1]
    piece = width // nodes
    masks = masks_of(local_count)
    bits = len(masks)
    rest = held - cap
    half = cap // 2
    order = near_first(nodes)
    items = [0] + order
    span = nodes // GROUPS
    total = span * local_count * cap
    copies = []
    sends = []

    def local_copy(src, dst):
        copy = pltpu.make_async_copy(src, dst, copy_sem.at[len(copies)])
        copy.start()
        copies.append(copy)
        return copy

    def remote(src, dst, device):
        i = len(sends)
        copy = pltpu.make_async_remote_copy(
            src_ref=src, dst_ref=dst, send_sem=send_sem.at[i], recv_sem=recv_sem.at[i],
            device_id=device, device_id_type=MESH,
        )
        copy.start()
        sends.append(copy)
        return copy

    loads = [local_copy(w, wbuf.at[i]) for i, w in enumerate((w0, w1, w2, w3, w4, w5))]

    barrier = pltpu.get_barrier_semaphore()
    for r in range(1, nodes):
        pl.semaphore_signal(
            barrier, inc=1, device_id=(lax.rem(n + r, nodes), l), device_id_type=MESH
        )
    for mask in masks:
        pl.semaphore_signal(barrier, inc=1, device_id=(n, l ^ mask), device_id_type=MESH)

    pick, meta, absent, meta_rest = routing_plan(ids[...], gates[...], n, nodes, cap)
    pick_out[...] = pick.astype(BF16)
    pick_b, absent_b = pick.astype(BF16), absent.astype(BF16)

    def place(r, columns, values):
        if r == 0:
            rows[0, 0, :, columns] = values
        else:
            away[r - 1, :, columns] = values

    tile = width // 7
    for source, base in ((tok, 0), (grad, width)):
        for c in range(7):
            chosen = dot(pick_b, source[:, c * tile : (c + 1) * tile])
            for r in range(nodes):
                place(
                    r, pl.ds(base + c * tile, tile),
                    chosen[r * cap : (r + 1) * cap].astype(BF16),
                )
    for r in range(nodes):
        place(r, pl.ds(2 * width, LANES), meta[r * cap : (r + 1) * cap].astype(BF16))
        start = pl.multiple_of(lax.rem(n + r, nodes) * piece, LANES)
        these = absent_b[r * rest : (r + 1) * rest]
        mine[r, :, 0:piece] = dot(these, tok[:, pl.ds(start, piece)]).astype(BF16)
        mine[r, :, piece : 2 * piece] = dot(these, grad[:, pl.ds(start, piece)]).astype(BF16)
        mine[r, :, 2 * piece :] = meta_rest[r * rest : (r + 1) * rest].astype(BF16)

    pl.semaphore_wait(barrier, nodes - 1 + bits)

    arrived = {}
    buffers = {"rows": (rows, width), "ext": (ext, piece)}

    def pass_on(name, k, p, columns):
        buf, _ = buffers[name]
        for b in range(2, bits):
            if p < 1 << b:
                q = p + (1 << b)
                arrived.setdefault((name, k, q), []).append((columns, remote(
                    buf.at[k, p, :, columns], buf.at[k, q, :, columns], (n, l ^ masks[b])
                )))

    def own(name, k):
        buf, _ = buffers[name]
        for b in range(2):
            arrived[name, k, 1 << b] = [(None, remote(
                buf.at[k, 0], buf.at[k, 1 << b], (n, l ^ masks[b])
            ))]
        pass_on(name, k, 0, slice(None))

    def forward(name, k):
        buf, split = buffers[name]
        ends = buf.shape[-1]
        parts = (pl.ds(0, split), pl.ds(split, ends - split))
        for p, over in ((1, 1), (2, 0)):
            for _, copy in arrived[name, k, p]:
                copy.wait_recv()
            columns = parts[p - 1]
            arrived.setdefault((name, k, 3), []).append((columns, remote(
                buf.at[k, p, :, columns], buf.at[k, 3, :, columns], (n, l ^ masks[over])
            )))
            pass_on(name, k, p, slice(None))

    def corner(name, k):
        for p in range(3, local_count // 2):
            for columns, copy in list(arrived[name, k, p]):
                copy.wait_recv()
                pass_on(name, k, p, columns)

    def complete(name, k):
        for p in range(local_count // 2, local_count):
            for _, copy in arrived[name, k, p]:
                copy.wait_recv()

    entering = {}
    own("rows", 0)
    for s in order:
        entering["rows", s] = remote(
            away.at[nodes - s - 1], rows.at[items.index(s), 0],
            (lax.rem(n + nodes - s, nodes), l),
        )
    for s in order:
        entering["ext", s] = remote(
            mine.at[nodes - s], ext.at[items.index(s), 0], (lax.rem(n + nodes - s, nodes), l)
        )
    ext_own = local_copy(mine.at[0], ext.at[0, 0])

    def enter(name, k):
        entering[name, items[k]].wait_recv()
        own(name, k)

    expert = l // (local_count // E_NODE)
    slots = iota((total, 1), 0) & (cap - 1)
    is_shared = flag(slots < half)
    deep = width // 7

    def chunk(g, columns):
        return rows[g * span : (g + 1) * span, :, :, columns].reshape(total, -1)

    def ffn(g):
        for i in range(6):
            pre[i] = jnp.zeros((total, units), F32)

        def step(c, carry):
            at = pl.multiple_of(c * deep, LANES)
            left_t = chunk(g, pl.ds(at, deep))
            left_g = chunk(g, pl.ds(width + at, deep))
            for i, left in enumerate((left_t, left_t, left_g) * 2):
                pre[i] += dot(left, wbuf[i, pl.ds(at, deep), :])
            return carry

        lax.fori_loop(0, 7, step, 0)
        table = chunk(g, pl.ds(2 * width, LANES)).astype(F32)
        weight = jnp.where(expert == 0, table[:, 0:1], table[:, 1:2])
        gg, gu, gh, product = ffn_backward(pre[0], pre[1], pre[2], weight)
        sg, su, sh, _ = ffn_backward(pre[3], pre[4], pre[5], is_shared)
        span_rows = pl.ds(g * total, total)
        for i, value in enumerate((gg, gu, gh)):
            grads_out[span_rows, i * units : (i + 1) * units] = value
        score = jnp.sum(product, axis=1, keepdims=True)
        lanes = iota((total, LANES), 1)
        score = jnp.where(lanes == expert, score, 0.0)
        part[g * span : (g + 1) * span, :, :, width:] = score.reshape(
            span, local_count, cap, LANES
        ).astype(BF16)
        kept = total * half // cap
        shift, low = cap.bit_length() - 1, half.bit_length() - 1
        j, h = iota((kept, total), 0), iota((kept, total), 1)
        compact = flag(h == ((j >> low) << shift) + (j & (half - 1))).astype(BF16)
        for i, value in enumerate((sg, su, sh)):
            packed[g, :, i * units : (i + 1) * units] = dot(compact, value).astype(BF16)
        return (gg, gu, sg, su)

    def spread_dx(g, values):
        gg, gu, sg, su = values

        def step(c, carry):
            at = pl.multiple_of(c * deep, LANES)
            for sub in range(2):
                size = deep // 2
                cols = pl.ds(pl.multiple_of(at + sub * size, LANES), size)
                total_dx = (
                    contract_last(gg, wbuf[0, cols, :]) + contract_last(gu, wbuf[1, cols, :])
                    + contract_last(sg, wbuf[3, cols, :]) + contract_last(su, wbuf[4, cols, :])
                )
                part[g * span : (g + 1) * span, :, :, cols] = total_dx.reshape(
                    span, local_count, cap, size
                ).astype(BF16)
            return carry

        lax.fori_loop(0, 7, step, 0)

    def send_packs(g):
        local_copy(packed.at[g], packs.at[0, g])
        for r in range(1, nodes):
            waits.append(remote(
                packed.at[g], packs.at[nodes - r, g], (lax.rem(n + r, nodes), l)
            ))

    waits = []
    full = part.shape[-1]
    cut = width // 2
    sides = (pl.ds(0, cut), pl.ds(cut, full - cut))
    everything = pl.ds(0, full)
    flight = {}
    upper = bits - 2

    def moves(stage):
        if stage < upper:
            b = bits - 1 - stage
            return [(1 << b, 1 << b, everything, masks[b], 1 << b)]
        if stage == upper:
            return [
                (1, 1, sides[0], masks[0], 1), (3, 1, sides[0], masks[0], 1),
                (2, 2, sides[1], masks[1], 2),
            ]
        return [(2, 1, sides[0], masks[1], 2), (1, 1, sides[1], masks[0], 1)]

    def reduce_start(g, stage):
        for k in range(g * span, (g + 1) * span):
            flight[k, stage] = [
                remote(
                    part.at[k, pl.ds(p, size), :, columns],
                    land.at[k, pl.ds(p, size), :, columns], (n, l ^ mask),
                )
                for p, size, columns, mask, _ in moves(stage)
            ]

    def reduce_settle(g, stage):
        for k in range(g * span, (g + 1) * span):
            for (p, size, columns, _, gap), copy in zip(moves(stage), flight[k, stage]):
                copy.wait_recv()

                def add(i, carry, k=k, p=p, gap=gap, columns=columns):
                    there = land[k, p + i, :, columns].astype(F32)
                    here = part[k, p + i - gap, :, columns].astype(F32)
                    part[k, p + i - gap, :, columns] = (here + there).astype(BF16)
                    return carry

                lax.fori_loop(0, size, add, 0)

    def go_home(g):
        for k in range(g * span, (g + 1) * span):
            s = items[k]
            if s == 0:
                local_copy(part.at[k, 0], back.at[0])
            else:
                waits.append(remote(
                    part.at[k, 0], back.at[nodes - s], (lax.rem(n + s, nodes), l)
                ))

    for k in range(nodes):
        if k > 0:
            enter("rows", k)
            forward("rows", k - 1)
        if k > 1:
            corner("rows", k - 2)
    for load in loads:
        load.wait()
    for k in range(span):
        if k == nodes - 2:
            corner("rows", k)
        complete("rows", k)
    values = ffn(0)
    send_packs(0)
    forward("rows", nodes - 1)
    corner("rows", nodes - 2)
    spread_dx(0, values)
    corner("rows", nodes - 1)
    reduce_start(0, 0)
    ext_own.wait()
    own("ext", 0)
    for k in range(1, nodes):
        enter("ext", k)
    for k in range(span, nodes):
        complete("rows", k)
    for k in range(nodes):
        local_copy(rows.at[k], rows_out.at[k])
    values = ffn(1)
    send_packs(1)
    reduce_settle(0, 0)
    reduce_start(0, 1)
    spread_dx(1, values)
    reduce_start(1, 0)
    for k in range(nodes):
        forward("ext", k)
    for stage in range(1, upper + 2):
        reduce_settle(0, stage)
        if stage < upper + 1:
            reduce_start(0, stage + 1)
        reduce_settle(1, stage - 1)
        reduce_start(1, stage)
    go_home(0)
    for k in range(nodes):
        corner("ext", k)
    reduce_settle(1, upper + 1)
    go_home(1)
    for k in range(nodes):
        complete("ext", k)
    for copy in waits:
        copy.wait_recv()
    for copy in copies[len(loads):]:
        if copy is not ext_own:
            copy.wait()
    for copy in sends:
        copy.wait_send()


def main_call(nodes, local_count, cap, tok, grad, ids, gates, weights):
    held, width = tok.shape
    units = weights[0].shape[1]
    rest, piece = held - cap, width // nodes
    span = nodes // GROUPS
    total = span * local_count * cap
    kept = total // 2
    full, wide, narrow = width + LANES, 2 * width + LANES, 2 * piece + LANES
    vmem = pl.BlockSpec(memory_space=pltpu.VMEM)
    hbm = pl.BlockSpec(memory_space=pl.ANY)
    shape = jax.ShapeDtypeStruct
    bits = local_count.bit_length() - 1
    gathers = 4
    for b in range(2, bits):
        gathers += (1 << b) + 1 + (b - 2) * 2
    gathers = 4 + sum(5 * 2 ** (b - 2) for b in range(2, bits))
    reduces = (bits - 2) + 5
    count = nodes * (2 * gathers + reduces) + (nodes - 1) * (3 + GROUPS)
    return pl.pallas_call(
        functools.partial(main_kernel, nodes, local_count, cap),
        out_shape=[
            shape((nodes, local_count, cap, wide), BF16),
            shape((nodes * local_count * cap, 3 * units), BF16),
            shape((nodes, GROUPS, kept, 3 * units), BF16),
            shape((nodes, local_count, rest, narrow), BF16),
            shape((nodes, cap, full), BF16),
            shape((nodes * cap, held), BF16),
        ],
        in_specs=[vmem] * 4 + [hbm] * 6,
        out_specs=[hbm, vmem, hbm, hbm, hbm, vmem],
        scratch_shapes=[
            pltpu.VMEM((nodes, local_count, cap, wide), BF16),
            pltpu.VMEM((nodes - 1, cap, wide), BF16),
            pltpu.VMEM((nodes, rest, narrow), BF16),
            pltpu.VMEM((6, width, units), BF16),
            pltpu.VMEM((nodes, local_count, cap, full), BF16),
            pltpu.VMEM((nodes, local_count, cap, full), BF16),
            pltpu.VMEM((6, total, units), F32),
            pltpu.VMEM((GROUPS, kept, 3 * units), BF16),
            pltpu.SemaphoreType.DMA((count,)),
            pltpu.SemaphoreType.DMA((count,)),
            pltpu.SemaphoreType.DMA((6 + 1 + GROUPS + nodes + 1,)),
        ],
        compiler_params=pltpu.CompilerParams(
            collective_id=0, has_side_effects=True, vmem_limit_bytes=67043328
        ),
        name="exchange",
    )(tok, grad, ids, gates, *weights)


def finish_kernel(
    nodes, local_count, cap, rest, order,
    where_ref, t_rows, g_rows, r_meta, t_piece, g_piece, t_ext, g_ext, e_meta,
    grads, packs, back, score, pick, ids,
    dw_g, dw_u, dw_d, ds_g, ds_u, ds_d, dx, dgates,
    near, far,
):
    units = dw_g.shape[1]
    half = cap // 2
    rows = nodes * cap
    seats = local_count * half
    items = [0] + order
    step = pl.program_id(0)

    @pl.when(step == 0)
    def _():
        shift, low = cap.bit_length() - 1, half.bit_length() - 1
        columns = nodes * seats
        seat = local_count.bit_length() - 1 + low
        h, j = iota((rows, columns), 0), iota((rows, columns), 1)
        widen = flag(
            ((h >> shift) == (j >> seat)) & ((h & (cap - 1)) == (j & (half - 1)))
        ).astype(BF16)
        block_of = (iota((1, columns), 1) & (seats - 1)) >> low
        for k, s in enumerate(items):
            pieces = []
            for r in range(nodes):
                at = (((s + r) % nodes) * nodes + items.index((nodes - r) % nodes)) * seats
                pieces.append(packs[at : at + seats, :])
            table = jnp.concatenate(pieces, axis=0)
            for meta, out, size in ((r_meta, near, cap), (e_meta, far, rest)):
                height = local_count * size
                perm = meta[k * height : (k + 1) * height, PERM : PERM + rows]
                owner = jnp.zeros((height, 1), I32)
                for p in range(1, local_count):
                    owner = owner + jnp.where(iota((height, 1), 0) >= p * size, 1, 0)
                full = jnp.where(owner == block_of, dot(perm, widen), 0.0).astype(BF16)
                out[k * height : (k + 1) * height, :] = dot(full, table).astype(BF16)
        n = where_ref[0]
        pick_t = contract_first(
            pick[...], flag(iota((rows, rows), 0) == iota((rows, rows), 1)).astype(BF16)
        )
        held = pick_t.shape[0]
        total = jnp.zeros((held, dgates.shape[1]), F32)
        rel = (ids[...] >> 1) - n
        rel = jnp.where(rel < 0, rel + nodes, rel)
        which = ids[...] & 1
        for k in range(dgates.shape[1]):
            here = (iota((held, rows), 1) >> shift) == rel[:, k : k + 1]
            found = dot(jnp.where(here, pick_t, 0.0).astype(BF16), score[...])
            found = jnp.where(iota((held, LANES), 1) == which[:, k : k + 1], found, 0.0)
            value = jnp.sum(found, axis=1, keepdims=True)
            total = jnp.where(iota((held, dgates.shape[1]), 1) == k, value, total)
        dgates[...] = total

    t, g = t_rows[...], g_rows[...]
    dw_g[...] = contract_first(t, grads[:, 0:units]).astype(BF16)
    dw_u[...] = contract_first(t, grads[:, units : 2 * units]).astype(BF16)
    dw_d[...] = contract_first(g, grads[:, 2 * units :]).astype(BF16)
    t_near, g_near, t_far, g_far = t_piece[...], g_piece[...], t_ext[...], g_ext[...]
    for i, (out, a, b) in enumerate((
        (ds_g, t_near, t_far), (ds_u, t_near, t_far), (ds_d, g_near, g_far),
    )):
        cols = slice(i * units, (i + 1) * units)
        out[...] = (contract_first(a, near[:, cols]) + contract_first(b, far[:, cols])).astype(
            BF16
        )
    dx[...] = contract_first(pick[...], back[...]).astype(BF16)


def finish_call(nodes, local_count, cap, n, rows, ext, grads, packs, back, pick, ids, width):
    units = grads.shape[1] // 3
    held = ids.shape[0]
    rest, piece = held - cap, width // nodes
    count = nodes * local_count * cap
    far_count = nodes * local_count * rest
    slots = nodes * cap
    blocks = piece // LANES
    steps = blocks // 2 if blocks % 2 == 0 else blocks
    tile, slim = width // steps, piece // steps
    rows = rows.reshape(count, -1)
    ext = ext.reshape(far_count, -1)
    back = back.reshape(slots, -1)
    packs = packs.reshape(-1, packs.shape[-1])

    def whole(shape):
        return pl.BlockSpec(shape, lambda j, n: (0,) * len(shape))

    def band(height, size, start):
        return pl.BlockSpec((height, size), lambda j, n: (0, start + j))

    def fixed(height, at):
        return pl.BlockSpec((height, LANES), lambda j, n: (0, at))

    def here(start):
        return pl.BlockSpec((count, slim), lambda j, n: (0, start + n[0] * steps + j))

    def out_rows(size):
        return pl.BlockSpec((size, units), lambda j, n: (j, 0))

    shape = jax.ShapeDtypeStruct
    flops = 2 * count * width * units * 3 + 2 * (count + far_count) * piece * units * 3
    return pl.pallas_call(
        functools.partial(finish_kernel, nodes, local_count, cap, rest, near_first(nodes)),
        grid_spec=pltpu.PrefetchScalarGridSpec(
            num_scalar_prefetch=1,
            grid=(steps,),
            in_specs=[
                band(count, tile, 0), band(count, tile, steps), fixed(count, 2 * width // LANES),
                here(0), here(width // slim),
                band(far_count, slim, 0), band(far_count, slim, steps),
                fixed(far_count, 2 * piece // LANES),
                whole(grads.shape), whole(packs.shape),
                band(slots, tile, 0), fixed(slots, width // LANES),
                whole(pick.shape), whole(ids.shape),
            ],
            out_specs=[out_rows(tile)] * 3 + [out_rows(slim)] * 3 + [
                pl.BlockSpec((held, tile), lambda j, n: (0, j)), whole(ids.shape),
            ],
            scratch_shapes=[
                pltpu.VMEM((count, 3 * units), BF16),
                pltpu.VMEM((far_count, 3 * units), BF16),
            ],
        ),
        out_shape=[shape((width, units), BF16)] * 3 + [shape((piece, units), BF16)] * 3 + [
            shape((held, width), BF16), shape(ids.shape, F32),
        ],
        cost_estimate=pl.CostEstimate(
            flops=flops, bytes_accessed=2 * (rows.size + 3 * width * units), transcendentals=0
        ),
        name="finish",
    )(n, rows, rows, rows, rows, rows, ext, ext, ext, grads, packs, back, back, pick, ids)


def local(tokens, grad_out, gates, expert_ids, w_gate, w_up, w_down, s_gate, s_up, s_down):
    held, width = tokens.shape
    nodes, locals_ = lax.axis_size("node"), lax.axis_size("local")
    cap = 2 * held // nodes
    weights = (w_gate[0], w_up[0], w_down[0], s_gate, s_up, s_down)
    rows, grads, packs, ext, back, pick = main_call(
        nodes, locals_, cap, tokens, grad_out, expert_ids, gates, weights
    )
    n = lax.axis_index("node").astype(I32).reshape(1)
    dw_g, dw_u, dw_d, ds_g, ds_u, ds_d, dx, dgates = finish_call(
        nodes, locals_, cap, n, rows, ext, grads, packs, back, pick, expert_ids, width
    )
    return (dx, dgates, dw_g[None], dw_u[None], dw_d[None], ds_g, ds_u, ds_d)


def solution(mesh):
    token = P(("node", "local"), None)
    routed = P("node", None, "local")
    shared = P(None, "local")
    shared_out = P("node", "local")
    return jax.shard_map(
        local,
        mesh=mesh,
        in_specs=(token,) * 4 + (routed,) * 3 + (shared,) * 3,
        out_specs=(token,) * 2 + (routed,) * 3 + (shared_out,) * 3,
        check_vma=False,
    )
```

```python
import functools
import math

import jax
import jax.numpy as jnp
from jax import lax
from jax.experimental import pallas as pl
from jax.experimental.pallas import tpu as pltpu
from jax.sharding import PartitionSpec as P

E_NODE = 2
LANES = 128
PERM = 64
MESH = pl.DeviceIdType.MESH
BF16, F32, I32 = jnp.bfloat16, jnp.float32, jnp.int32


def masks_of(local_count):
    bits = local_count.bit_length() - 1
    return [1 << b for b in range(1, bits)] + [1]


def order_of(node_count):
    return [0, 2, 1, 3] if node_count == 4 else list(range(node_count))


def spans_of(node_count):
    return [(0, node_count // 2), (node_count // 2, node_count - node_count // 2)]


def dot(left, right):
    return jnp.dot(left, right, preferred_element_type=F32)


def contract_first(left, right):
    return lax.dot_general(left, right, (((0,), (0,)), ((), ())), preferred_element_type=F32)


def contract_last(left, right):
    return lax.dot_general(left, right, (((1,), (1,)), ((), ())), preferred_element_type=F32)


def iota(shape, axis):
    return lax.broadcasted_iota(I32, shape, axis)


def flag(values):
    return jnp.where(values, 1.0, 0.0).astype(F32)


def routing_plan(ids, gates, n, nodes, cap):
    held = ids.shape[1]
    shift = cap.bit_length() - 1
    rest = held - cap
    rows, rest_rows = nodes * cap, nodes * rest
    half = cap // 2
    gates = gates.astype(F32)
    rel = (ids >> 1) ^ n
    which = ids & 1
    count = ids.shape[0]
    lane_node = iota((nodes, held), 0)
    hit = jnp.zeros((nodes, held), F32)
    gate_of = [jnp.zeros((nodes, held), F32) for _ in range(E_NODE)]
    for k in range(count):
        here = lane_node == rel[k : k + 1, :]
        hit = jnp.maximum(hit, flag(here))
        for e in range(E_NODE):
            named = here & (which[k : k + 1, :] == e)
            gate_of[e] = gate_of[e] + jnp.where(named, gates[k : k + 1, :], 0.0)
    upper = flag(iota((held, held), 0) <= iota((held, held), 1))
    rank = dot(hit, upper) - 1.0
    spread = flag((iota((rows, nodes), 0) >> shift) == iota((rows, nodes), 1))
    slot = (iota((rows, held), 0) & (cap - 1)).astype(F32)
    first = flag((dot(spread, hit) > 0.5) & (dot(spread, rank) == slot))

    row, lane = iota((rows, rows), 0), iota((rows, rows), 1)
    unit = flag(row == lane)
    ends = contract_last(first, first) * (1.0 - unit)
    pairs = flag((row ^ 1) == lane)
    reach = unit + dot(ends, pairs)
    for _ in range((held - 1).bit_length()):
        reach = jnp.minimum(dot(reach, reach), 1.0)
    number = lane.astype(F32)
    far = dot(ends, reach)
    label = jnp.min(jnp.where(reach > 0.5, number, float(rows)), axis=1, keepdims=True)
    other = jnp.min(jnp.where(far > 0.5, number, float(rows)), axis=1, keepdims=True)
    taken = flag(label < other)
    same = (row >> shift) == (lane >> shift)
    before = flag(same & (lane < row))
    taken_wide = jnp.broadcast_to(taken, (rows, LANES))
    taken_rank = dot(before, taken_wide)[:, 0:1]
    left_rank = dot(before, 1.0 - taken_wide)[:, 0:1]
    place = jnp.where(taken > 0.5, taken_rank, left_rank + float(half))
    move = flag(same & (place == (lane & (cap - 1)).astype(F32)))
    pick = contract_first(move, first)

    assigned = pick * flag((iota((rows, held), 0) & (cap - 1)) < half)
    weights = [
        jnp.sum(pick * dot(spread, gate_of[e]), axis=1, keepdims=True) for e in range(E_NODE)
    ]
    spot = flag(iota((rows, LANES), 1) == iota((rows, LANES), 0) + PERM)
    lanes = iota((rows, LANES), 1)
    meta = dot(contract_last(pick, assigned), spot)
    for e in range(E_NODE):
        meta = meta + jnp.where(lanes == e, weights[e], 0.0)

    shape = (rest_rows, held)
    block = jnp.zeros(shape, I32)
    for r in range(1, nodes):
        block = block + jnp.where(iota(shape, 0) >= r * rest, 1, 0)
    within = (iota(shape, 0) - block * rest).astype(F32)
    spread_rest = flag(block[:, 0:1] == iota((rest_rows, nodes), 1))
    away = 1.0 - hit
    away_rank = dot(away, upper) - 1.0
    absent = flag((dot(spread_rest, away) > 0.5) & (dot(spread_rest, away_rank) == within))
    meta_rest = dot(contract_last(absent, assigned), spot)
    return pick, meta, absent, meta_rest


def silu_parts(pre_gate):
    sig = jax.nn.sigmoid(pre_gate)
    return (pre_gate * sig, sig * (1.0 + pre_gate * (1.0 - sig)))


def ffn_backward(pre_gate, pre_up, upstream, weight):
    activ, slope = silu_parts(pre_gate)
    hidden = activ * pre_up
    scaled = weight * upstream
    grad_up = (scaled * activ).astype(BF16)
    grad_gate = (scaled * pre_up * slope).astype(BF16)
    weighted = (weight * hidden).astype(BF16)
    return (grad_gate, grad_up, weighted, hidden * upstream)


def main_kernel(
    nodes, local_count, cap,
    tok, grad, ids, gates, w0, w1, w2, w3, w4, w5,
    rows, ext, near, far, dw_g, dw_u, dw_d, back, pick_out,
    packs, away, mine, w_in, w_out, turned, part, land, pre, grads,
    send_sem, recv_sem, cross_send, cross_recv, load_sem,
):
    n, l = lax.axis_index("node"), lax.axis_index("local")
    held, width = tok.shape
    units = w0.shape[1]
    piece = width // nodes
    masks = masks_of(local_count)
    bits = len(masks)
    rest = held - cap
    half = cap // 2
    seats = local_count * half
    spans = spans_of(nodes)
    order = order_of(nodes)
    sends = []

    def remote(src, dst, device):
        i = len(sends)
        copy = pltpu.make_async_remote_copy(
            src_ref=src, dst_ref=dst, send_sem=send_sem.at[i], recv_sem=recv_sem.at[i],
            device_id=device, device_id_type=MESH,
        )
        copy.start()
        sends.append(copy)
        return copy

    barrier = pltpu.get_barrier_semaphore()
    for r in range(1, nodes):
        pl.semaphore_signal(barrier, inc=1, device_id=(n ^ r, l), device_id_type=MESH)
    for mask in masks:
        pl.semaphore_signal(barrier, inc=1, device_id=(n, l ^ mask), device_id_type=MESH)

    loads = []
    stack = ((w0, w_in, 0), (w1, w_in, 1), (w3, w_in, 2), (w4, w_in, 3), (w2, w_out, 0), (w5, w_out, 1))
    for i, (w, buf, at) in enumerate(stack):
        load = pltpu.make_async_copy(w, buf.at[:, at * units : (at + 1) * units], load_sem.at[i])
        load.start()
        loads.append(load)

    pick, meta, absent, meta_rest = routing_plan(ids[...], gates[...], n, nodes, cap)
    pick_out[...] = pick.astype(BF16)
    pick_b, absent_b = pick.astype(BF16), absent.astype(BF16)

    def place(r, columns, values):
        if r == 0:
            rows[0, 0, :, columns] = values
        else:
            away[r - 1, :, columns] = values

    tile = width // 7
    for source, base in ((tok, 0), (grad, width)):
        for c in range(7):
            chosen = dot(pick_b, source[:, c * tile : (c + 1) * tile])
            for r in range(nodes):
                place(
                    r, pl.ds(base + c * tile, tile),
                    chosen[r * cap : (r + 1) * cap].astype(BF16),
                )
    for r in range(nodes):
        place(r, pl.ds(2 * width, LANES), meta[r * cap : (r + 1) * cap].astype(BF16))

    pl.semaphore_wait(barrier, nodes - 1 + bits)

    arrived = {}
    buffers = {"rows": (rows, width), "ext": (ext, piece)}

    def pass_on(name, k, p, columns):
        buf, _ = buffers[name]
        for b in range(2, bits):
            if p < 1 << b:
                q = p + (1 << b)
                arrived.setdefault((name, k, q), []).append((columns, remote(
                    buf.at[k, p, :, columns], buf.at[k, q, :, columns], (n, l ^ masks[b])
                )))

    def own(name, k):
        buf, _ = buffers[name]
        for b in range(2):
            arrived[name, k, 1 << b] = [(None, remote(
                buf.at[k, 0], buf.at[k, 1 << b], (n, l ^ masks[b])
            ))]
        pass_on(name, k, 0, slice(None))

    def forward(name, k):
        buf, split = buffers[name]
        ends = buf.shape[-1]
        parts = (pl.ds(0, split), pl.ds(split, ends - split))
        for p, over in ((1, 1), (2, 0)):
            for _, copy in arrived[name, k, p]:
                copy.wait_recv()
            columns = parts[p - 1]
            arrived.setdefault((name, k, 3), []).append((columns, remote(
                buf.at[k, p, :, columns], buf.at[k, 3, :, columns], (n, l ^ masks[over])
            )))
            pass_on(name, k, p, slice(None))

    def corner(name, k):
        for p in range(3, local_count // 2):
            for columns, copy in list(arrived[name, k, p]):
                copy.wait_recv()
                pass_on(name, k, p, columns)

    def complete(name, k):
        for p in range(local_count // 2, local_count):
            for _, copy in arrived[name, k, p]:
                copy.wait_recv()

    entering = {}
    own("rows", 0)
    for k in range(1, nodes):
        r = order[k]
        entering["rows", k] = pltpu.make_async_remote_copy(
            src_ref=away.at[r - 1], dst_ref=rows.at[k, 0],
            send_sem=cross_send.at[k - 1], recv_sem=cross_recv.at[k - 1],
            device_id=(n ^ r, l), device_id_type=MESH,
        )
    for k in range(1, nodes):
        entering["rows", k].start()

    for r in range(nodes):
        start = pl.multiple_of((n ^ r) * piece, LANES)
        these = absent_b[r * rest : (r + 1) * rest]
        values = [
            (pl.ds(0, piece), dot(these, tok[:, pl.ds(start, piece)])),
            (pl.ds(piece, piece), dot(these, grad[:, pl.ds(start, piece)])),
            (pl.ds(2 * piece, LANES), meta_rest[r * rest : (r + 1) * rest]),
        ]
        for columns, value in values:
            if r == 0:
                ext[0, 0, :, columns] = value.astype(BF16)
            else:
                mine[r - 1, :, columns] = value.astype(BF16)

    def cross_ext():
        for k in range(1, nodes):
            r = order[k]
            entering["ext", k] = remote(mine.at[r - 1], ext.at[k, 0], (n ^ r, l))

    def enter(name, k):
        entering[name, k].wait_recv()
        own(name, k)

    expert = l // (local_count // E_NODE)
    deep = width // 7
    block = local_count * cap

    def chunk(k0, m, columns):
        return rows[k0 : k0 + m, :, :, columns].reshape(m * block, -1)

    def ffn(g):
        k0, m = spans[g]
        total = m * block
        pre[0:total, :] = jnp.zeros((total, 6 * units), F32)

        def step(c, carry):
            at = pl.multiple_of(c * deep, LANES)
            here = pl.ds(at, deep)
            pre[0:total, 0 : 4 * units] += dot(chunk(k0, m, here), w_in[here, :])
            left_g = chunk(k0, m, pl.ds(width + at, deep))
            pre[0:total, 4 * units :] += dot(left_g, w_out[here, :])
            return carry

        lax.fori_loop(0, 7, step, 0)
        table = chunk(k0, m, pl.ds(2 * width, LANES)).astype(F32)
        weight = jnp.where(expert == 0, table[:, 0:1], table[:, 1:2])
        is_shared = flag((iota((total, 1), 0) & (cap - 1)) < half)
        p, q, p_s, q_s, u, u_s = (pre[0:total, i * units : (i + 1) * units] for i in range(6))
        gg, gu, gh, product = ffn_backward(p, q, u, weight)
        sg, su, sh, _ = ffn_backward(p_s, q_s, u_s, is_shared)
        for i, value in enumerate((gg, gu, sg, su, gh)):
            grads[k0 * block : (k0 + m) * block, i * units : (i + 1) * units] = value
        score = jnp.sum(product, axis=1, keepdims=True)
        lanes = iota((total, LANES), 1)
        score = jnp.where(lanes == expert, score, 0.0)
        part[k0 : k0 + m, :, :, width:] = score.reshape(m, local_count, cap, LANES).astype(BF16)
        kept = m * seats
        shift, low = cap.bit_length() - 1, half.bit_length() - 1
        j, h = iota((kept, total), 0), iota((kept, total), 1)
        compact = flag(h == ((j >> low) << shift) + (j & (half - 1))).astype(BF16)
        for i, value in enumerate((sg, su, sh)):
            packs[0, k0 * seats : (k0 + m) * seats, i * units : (i + 1) * units] = dot(
                compact, value
            ).astype(BF16)

    turns = (dw_g, dw_u, dw_d, turned)

    def turn(i):
        loads[i].wait()
        eye = flag(iota((units, units), 0) == iota((units, units), 1)).astype(BF16)
        group = 4

        def step(c, carry):
            for sub in range(group):
                at = pl.ds(pl.multiple_of((c * group + sub) * units, LANES), units)
                turns[i][at, :] = contract_last(
                    eye, w_in[at, i * units : (i + 1) * units]
                ).astype(BF16)
            return carry

        lax.fori_loop(0, width // units // group, step, 0)

    def spread_dx(g, side):
        k0, m = spans[g]
        these = slice(k0 * block, (k0 + m) * block)
        group = 2
        count = width // 2 // units // group

        def step(c, carry):
            for sub in range(group):
                at = pl.ds(pl.multiple_of((c * group + sub) * units, LANES), units)
                total_dx = sum(
                    dot(grads[these, i * units : (i + 1) * units], turns[i][at, :])
                    for i in range(4)
                )
                part[k0 : k0 + m, :, :, at] = total_dx.reshape(m, local_count, cap, units).astype(
                    BF16
                )
            return carry

        lax.fori_loop(count * side, count * (side + 1), step, 0)

    def weight_grad(i, begin, end):
        base, first, outs = ((0, 0, (dw_g, dw_u)), (width, 4, (dw_d,)))[i]
        right = slice(first * units, (first + len(outs)) * units)
        size = deep // 2

        def step(c, carry):
            at = pl.multiple_of(c * size, LANES)
            left = chunk(0, nodes, pl.ds(base + at, size))
            both = contract_first(left, grads[:, right]).astype(BF16)
            for o, out in enumerate(outs):
                out[pl.ds(at, size), :] = both[:, o * units : (o + 1) * units]
            return carry

        lax.fori_loop(begin, end, step, 0)

    def arrange(name):
        source, out, size = {"rows": (rows, near, cap), "ext": (ext, far, rest)}[name]
        shift, low = cap.bit_length() - 1, half.bit_length() - 1
        slots, columns = nodes * cap, nodes * seats
        seat = local_count.bit_length() - 1 + low
        h, j = iota((slots, columns), 0), iota((slots, columns), 1)
        widen = flag(
            ((h >> shift) == (j >> seat)) & ((h & (cap - 1)) == (j & (half - 1)))
        ).astype(BF16)
        block_of = (iota((1, columns), 1) & (seats - 1)) >> low
        height = local_count * size
        owner = jnp.zeros((height, 1), I32)
        for p in range(1, local_count):
            owner = owner + jnp.where(iota((height, 1), 0) >= p * size, 1, 0)
        meta = source.shape[-1] - LANES
        for k in range(nodes):
            table = jnp.concatenate([
                packs[order.index(order[k] ^ r), order.index(r) * seats : (order.index(r) + 1) * seats, :]
                for r in range(nodes)
            ], axis=0)
            perm = source[k, :, :, meta:].reshape(height, LANES)[:, PERM : PERM + slots]
            full = jnp.where(owner == block_of, dot(perm, widen), 0.0).astype(BF16)
            out[k * height : (k + 1) * height, :] = dot(full, table).astype(BF16)

    waits, packed = [], []

    def send_packs(g):
        k0, m = spans[g]
        these = pl.ds(k0 * seats, m * seats)
        for k in range(1, nodes):
            packed.append(remote(packs.at[0, these], packs.at[k, these], (n ^ order[k], l)))

    full = part.shape[-1]
    cut = width // 2
    sides = (pl.ds(0, cut), pl.ds(cut, full - cut))
    flight = {}
    upper = bits - 2
    last = upper + 1

    def moves(side, stage):
        if stage < upper:
            b = bits - 1 - stage
            return [(1 << b, 1 << b)], masks[b], 1 << b
        first = stage == upper
        if side == 0:
            return ([(1, 1), (3, 1)], masks[0], 1) if first else ([(2, 1)], masks[1], 2)
        return ([(2, 2)], masks[1], 2) if first else ([(1, 1)], masks[0], 1)

    def reduce_start(g, side, stage):
        blocks, mask, _ = moves(side, stage)
        k0, m = spans[g]
        flight[g, side, stage] = [
            (k, p, size, remote(
                part.at[k, pl.ds(p, size), :, sides[side]],
                land.at[k, pl.ds(p, size), :, sides[side]], (n, l ^ mask),
            ))
            for k in range(k0, k0 + m) for p, size in blocks
        ]

    def reduce_settle(g, side, stage):
        _, _, gap = moves(side, stage)
        columns = sides[side]
        for k, p, size, copy in flight[g, side, stage]:
            copy.wait_recv()

            def add(i, carry, k=k, p=p):
                there = land[k, p + i, :, columns].astype(F32)
                here = part[k, p + i - gap, :, columns].astype(F32)
                part[k, p + i - gap, :, columns] = (here + there).astype(BF16)
                return carry

            lax.fori_loop(0, size, add, 0)

    def reduce_next(g, side, stage):
        reduce_settle(g, side, stage)
        if stage < last:
            reduce_start(g, side, stage + 1)

    def go_home(g, side):
        k0, m = spans[g]
        columns = sides[side]
        for k in range(k0, k0 + m):
            if k == 0:
                back[0, :, columns] = part[0, 0, :, columns]
            else:
                waits.append(remote(
                    part.at[k, 0, :, columns], back.at[order[k], :, columns], (n ^ order[k], l)
                ))

    half_way = spans[1][0]
    turn(0)
    turn(1)
    forward("rows", 0)
    turn(2)
    corner("rows", 0)
    enter("rows", 1)
    turn(3)
    forward("rows", 1)
    for k in range(2, half_way):
        enter("rows", k)
        forward("rows", k)
        corner("rows", k - 1)
    for k in range(half_way, nodes):
        enter("rows", k)
    corner("rows", half_way - 1)
    cross_ext()
    for load in loads[4:]:
        load.wait()
    for k in range(half_way):
        complete("rows", k)
    ffn(0)
    send_packs(0)
    for k in range(half_way, nodes - 1):
        forward("rows", k)
    spread_dx(0, 0)
    reduce_start(0, 0, 0)
    forward("rows", nodes - 1)
    for k in range(half_way, nodes - 1):
        corner("rows", k)
    spread_dx(0, 1)
    reduce_start(0, 1, 0)
    corner("rows", nodes - 1)
    for side in range(2):
        reduce_next(0, side, 0)
    own("ext", 0)
    for k in range(1, nodes):
        enter("ext", k)
    for k in range(half_way, nodes):
        complete("rows", k)
    ffn(1)
    send_packs(1)
    spread_dx(1, 0)
    reduce_start(1, 0, 0)
    for side in range(2):
        reduce_next(0, side, 1)
    spread_dx(1, 1)
    reduce_start(1, 1, 0)
    todo = [(i, b, min(b + 3 + i, 14)) for i in range(2) for b in range(0, 14, 3 + i)]

    def fill(count):
        for _ in range(min(count, len(todo))):
            weight_grad(*todo.pop(0))

    reduce_next(1, 0, 0)
    fill(1)
    reduce_next(1, 1, 0)
    for stage in range(2, last + 1):
        fill(3)
        for side in range(2):
            reduce_next(0, side, stage)
    for side in range(2):
        go_home(0, side)
    for stage in range(1, last):
        fill(2)
        for side in range(2):
            reduce_next(1, side, stage)
    for k in range(nodes):
        forward("ext", k)
    fill(2)
    reduce_next(1, 0, last)
    go_home(1, 0)
    fill(1)
    reduce_next(1, 1, last)
    go_home(1, 1)
    for k in range(nodes):
        corner("ext", k)
    fill(len(todo))
    for copy in packed:
        copy.wait_recv()
    arrange("rows")
    for k in range(nodes):
        complete("ext", k)
    arrange("ext")
    for copy in waits:
        copy.wait_recv()
    for k in range(1, nodes):
        entering["rows", k].wait_send()
    for copy in sends:
        copy.wait_send()


def room(scratch):
    held = sum(math.prod(dims) * jnp.dtype(kind).itemsize for dims, kind in scratch)
    return held + held // 32 + 2 * 2**20


def main_call(nodes, local_count, cap, tok, grad, ids, gates, weights):
    held, width = tok.shape
    units = weights[0].shape[1]
    rest, piece = held - cap, width // nodes
    most = max(m for _, m in spans_of(nodes)) * local_count * cap
    total = nodes * local_count * cap
    full, wide, narrow = width + LANES, 2 * width + LANES, 2 * piece + LANES
    vmem = pl.BlockSpec(memory_space=pltpu.VMEM)
    hbm = pl.BlockSpec(memory_space=pl.ANY)
    bits = local_count.bit_length() - 1
    gathers = 4 + sum(5 * 2 ** (b - 2) for b in range(2, bits))
    reduces = 2 * (bits - 2) + 5
    count = nodes * (2 * gathers + reduces) + (nodes - 1) * (3 + len(spans_of(nodes)))
    part = (nodes, local_count, cap, full)
    scratch = [
        ((nodes, total // 2, 3 * units), BF16),
        ((nodes - 1, cap, wide), BF16),
        ((nodes - 1, rest, narrow), BF16),
        ((width, 4 * units), BF16),
        ((width, 2 * units), BF16),
        ((width, units), BF16),
        (part, BF16),
        (part, BF16),
        ((most, 6 * units), F32),
        ((total, 5 * units), BF16),
    ]
    results = [
        (nodes, local_count, cap, wide),
        (nodes, local_count, rest, narrow),
        (total, 3 * units),
        (nodes * local_count * rest, 3 * units),
    ] + [(width, units)] * 3 + [(nodes, cap, full), (nodes * cap, held)]
    return pl.pallas_call(
        functools.partial(main_kernel, nodes, local_count, cap),
        out_shape=[pltpu.VMEM(dims, BF16) for dims in results],
        in_specs=[vmem] * 4 + [hbm] * 6,
        out_specs=[vmem] * 9,
        scratch_shapes=[pltpu.VMEM(*entry) for entry in scratch] + [
            pltpu.SemaphoreType.DMA((count,)),
            pltpu.SemaphoreType.DMA((count,)),
            pltpu.SemaphoreType.DMA((nodes - 1,)),
            pltpu.SemaphoreType.DMA((nodes - 1,)),
            pltpu.SemaphoreType.DMA((6,)),
        ],
        compiler_params=pltpu.CompilerParams(
            collective_id=0, has_side_effects=True, vmem_limit_bytes=room(scratch)
        ),
        name="exchange",
    )(tok, grad, ids, gates, *weights)


def finish_kernel(
    cap,
    rows, ext, near, far, dw_g, dw_u, dw_d, back, pick, ids,
    out_g, out_u, out_d, ds_g, ds_u, ds_d, dx, dgates,
    ds, sem,
):
    n = lax.axis_index("node")
    width, units = dw_g.shape
    piece = ds.shape[1]
    slots = pick.shape[0]
    copies = []

    def store(src, dst):
        copy = pltpu.make_async_copy(src, dst, sem.at[len(copies)])
        copy.start()
        copies.append(copy)

    for src, dst in ((dw_g, out_g), (dw_u, out_u), (dw_d, out_d)):
        store(src, dst)

    size = piece // 7
    for i, count in enumerate((2, 1)):
        cols = slice(2 * i * units, (2 * i + count) * units)

        def step(c, carry, i=i, cols=cols, count=count):
            at = pl.multiple_of(c * size, LANES)
            there = pl.multiple_of(i * width + n * piece + at, LANES)
            a = rows[:, :, :, pl.ds(there, size)].reshape(near.shape[0], size)
            b = ext[:, :, :, pl.ds(i * piece + at, size)].reshape(far.shape[0], size)
            value = contract_first(a, near[:, cols]) + contract_first(b, far[:, cols])
            for o in range(count):
                ds[2 * i + o, pl.ds(at, size), :] = value[
                    :, o * units : (o + 1) * units
                ].astype(BF16)
            return carry

        lax.fori_loop(0, 7, step, 0)
        for o in range(count):
            store(ds.at[2 * i + o], (ds_g, ds_u, ds_d)[2 * i + o])

    flat = back[...].reshape(slots, back.shape[-1])
    tile = width // 7
    for c in range(7):
        cols = slice(c * tile, (c + 1) * tile)
        dx[:, cols] = contract_first(pick[...], flat[:, cols]).astype(BF16)
    score = flat[:, width:].astype(F32)
    rel = (ids[...] >> 1) ^ n
    which = ids[...] & 1
    seen = pick[...].astype(F32)
    row_node = iota(seen.shape, 0) >> (cap.bit_length() - 1)
    total = jnp.zeros(dgates.shape, F32)
    for k in range(dgates.shape[0]):
        value = jnp.where(which[k : k + 1, :] == 0, score[:, 0:1], score[:, 1:2])
        value = jnp.where(row_node == rel[k : k + 1, :], seen * value, 0.0)
        value = jnp.sum(value, axis=0, keepdims=True)
        total = jnp.where(iota(dgates.shape, 0) == k, value, total)
    dgates[...] = total
    for copy in copies:
        copy.wait()


def finish_call(nodes, cap, values, ids):
    width, units = values[4].shape
    vmem = pl.BlockSpec(memory_space=pltpu.VMEM)
    hbm = pl.BlockSpec(memory_space=pl.ANY)
    shape = jax.ShapeDtypeStruct
    piece = width // nodes
    scratch = [((3, piece, units), BF16)]
    return pl.pallas_call(
        functools.partial(finish_kernel, cap),
        in_specs=[vmem] * 10,
        out_specs=[hbm] * 6 + [vmem] * 2,
        out_shape=[shape((width, units), BF16)] * 3 + [shape((piece, units), BF16)] * 3 + [
            shape((ids.shape[1], width), BF16), shape(ids.shape, F32),
        ],
        scratch_shapes=[pltpu.VMEM(*entry) for entry in scratch] + [
            pltpu.SemaphoreType.DMA((6,)),
        ],
        compiler_params=pltpu.CompilerParams(vmem_limit_bytes=room(scratch)),
        name="finish",
    )(*values, ids)


def local(tokens, grad_out, gates, expert_ids, w_gate, w_up, w_down, s_gate, s_up, s_down):
    held, width = tokens.shape
    nodes, locals_ = lax.axis_size("node"), lax.axis_size("local")
    cap = 2 * held // nodes
    weights = (w_gate[0], w_up[0], w_down[0], s_gate, s_up, s_down)
    ids = expert_ids.T
    values = main_call(nodes, locals_, cap, tokens, grad_out, ids, gates.T, weights)
    dw_g, dw_u, dw_d, ds_g, ds_u, ds_d, dx, dgates = finish_call(
        nodes, cap, values, ids
    )
    return (dx, dgates.T, dw_g[None], dw_u[None], dw_d[None], ds_g, ds_u, ds_d)


def solution(mesh):
    token = P(("node", "local"), None)
    routed = P("node", None, "local")
    shared = P(None, "local")
    shared_out = P("node", "local")
    return jax.shard_map(
        local,
        mesh=mesh,
        in_specs=(token,) * 4 + (routed,) * 3 + (shared,) * 3,
        out_specs=(token,) * 2 + (routed,) * 3 + (shared_out,) * 3,
        check_vma=False,
    )
```

```python
import functools
import math

import jax
import jax.numpy as jnp
from jax import lax
from jax.experimental import pallas as pl
from jax.experimental.pallas import tpu as pltpu
from jax.sharding import PartitionSpec as P

E_NODE = 2
LANES = 128
PERM = 64
MESH = pl.DeviceIdType.MESH
BF16, F32, I32 = jnp.bfloat16, jnp.float32, jnp.int32


def masks_of(local_count):
    bits = local_count.bit_length() - 1
    return [1 << b for b in range(1, bits)] + [1]


def order_of(node_count):
    return [0, 2, 1, 3] if node_count == 4 else list(range(node_count))


def spans_of(node_count):
    return [(0, node_count // 2), (node_count // 2, node_count - node_count // 2)]


def dot(left, right):
    return jnp.dot(left, right, preferred_element_type=F32)


def contract_first(left, right):
    return lax.dot_general(left, right, (((0,), (0,)), ((), ())), preferred_element_type=F32)


def contract_last(left, right):
    return lax.dot_general(left, right, (((1,), (1,)), ((), ())), preferred_element_type=F32)


def iota(shape, axis):
    return lax.broadcasted_iota(I32, shape, axis)


def flag(values):
    return jnp.where(values, 1.0, 0.0).astype(F32)


def routing_plan(ids, gates, n, nodes, cap):
    held = ids.shape[1]
    shift = cap.bit_length() - 1
    rest = held - cap
    rows, rest_rows = nodes * cap, nodes * rest
    half = cap // 2
    gates = gates.astype(F32)
    rel = (ids >> 1) ^ n
    which = ids & 1
    count = ids.shape[0]
    lane_node = iota((nodes, held), 0)
    hit = jnp.zeros((nodes, held), F32)
    gate_of = [jnp.zeros((nodes, held), F32) for _ in range(E_NODE)]
    for k in range(count):
        here = lane_node == rel[k : k + 1, :]
        hit = jnp.maximum(hit, flag(here))
        for e in range(E_NODE):
            named = here & (which[k : k + 1, :] == e)
            gate_of[e] = gate_of[e] + jnp.where(named, gates[k : k + 1, :], 0.0)
    upper = flag(iota((held, held), 0) <= iota((held, held), 1))
    rank = dot(hit, upper) - 1.0
    spread = flag((iota((rows, nodes), 0) >> shift) == iota((rows, nodes), 1))
    slot = (iota((rows, held), 0) & (cap - 1)).astype(F32)
    first = flag((dot(spread, hit) > 0.5) & (dot(spread, rank) == slot))

    row, lane = iota((rows, rows), 0), iota((rows, rows), 1)
    unit = flag(row == lane)
    ends = contract_last(first, first) * (1.0 - unit)
    pairs = flag((row ^ 1) == lane)
    reach = unit + dot(ends, pairs)
    for _ in range((held - 1).bit_length()):
        reach = jnp.minimum(dot(reach, reach), 1.0)
    number = lane.astype(F32)
    far = dot(ends, reach)
    label = jnp.min(jnp.where(reach > 0.5, number, float(rows)), axis=1, keepdims=True)
    other = jnp.min(jnp.where(far > 0.5, number, float(rows)), axis=1, keepdims=True)
    taken = flag(label < other)
    same = (row >> shift) == (lane >> shift)
    before = flag(same & (lane < row))
    taken_wide = jnp.broadcast_to(taken, (rows, LANES))
    taken_rank = dot(before, taken_wide)[:, 0:1]
    left_rank = dot(before, 1.0 - taken_wide)[:, 0:1]
    place = jnp.where(taken > 0.5, taken_rank, left_rank + float(half))
    move = flag(same & (place == (lane & (cap - 1)).astype(F32)))
    pick = contract_first(move, first)

    assigned = pick * flag((iota((rows, held), 0) & (cap - 1)) < half)
    weights = [
        jnp.sum(pick * dot(spread, gate_of[e]), axis=1, keepdims=True) for e in range(E_NODE)
    ]
    spot = flag(iota((rows, LANES), 1) == iota((rows, LANES), 0) + PERM)
    lanes = iota((rows, LANES), 1)
    meta = dot(contract_last(pick, assigned), spot)
    for e in range(E_NODE):
        meta = meta + jnp.where(lanes == e, weights[e], 0.0)

    shape = (rest_rows, held)
    block = jnp.zeros(shape, I32)
    for r in range(1, nodes):
        block = block + jnp.where(iota(shape, 0) >= r * rest, 1, 0)
    within = (iota(shape, 0) - block * rest).astype(F32)
    spread_rest = flag(block[:, 0:1] == iota((rest_rows, nodes), 1))
    away = 1.0 - hit
    away_rank = dot(away, upper) - 1.0
    absent = flag((dot(spread_rest, away) > 0.5) & (dot(spread_rest, away_rank) == within))
    meta_rest = dot(contract_last(absent, assigned), spot)
    return pick, meta, absent, meta_rest


def silu_parts(pre_gate):
    sig = jax.nn.sigmoid(pre_gate)
    return (pre_gate * sig, sig * (1.0 + pre_gate * (1.0 - sig)))


def ffn_backward(pre_gate, pre_up, upstream, weight):
    activ, slope = silu_parts(pre_gate)
    hidden = activ * pre_up
    scaled = weight * upstream
    grad_up = (scaled * activ).astype(BF16)
    grad_gate = (scaled * pre_up * slope).astype(BF16)
    weighted = (weight * hidden).astype(BF16)
    return (grad_gate, grad_up, weighted, hidden * upstream)


def main_kernel(
    nodes, local_count, cap,
    tok, grad, ids, gates, w0, w1, w2, w3, w4, w5,
    rows, ext, near, far, dw_g, dw_u, dw_d, back, pick_out,
    packs, away, mine, w_in, w_out, turned, part, land, pre, grads,
    send_sem, recv_sem, cross_send, cross_recv, load_sem,
):
    n, l = lax.axis_index("node"), lax.axis_index("local")
    held, width = tok.shape
    units = w0.shape[1]
    piece = width // nodes
    masks = masks_of(local_count)
    bits = len(masks)
    rest = held - cap
    half = cap // 2
    seats = local_count * half
    spans = spans_of(nodes)
    order = order_of(nodes)
    sends = []

    def remote(src, dst, device):
        i = len(sends)
        copy = pltpu.make_async_remote_copy(
            src_ref=src, dst_ref=dst, send_sem=send_sem.at[i], recv_sem=recv_sem.at[i],
            device_id=device, device_id_type=MESH,
        )
        copy.start()
        sends.append(copy)
        return copy

    barrier = pltpu.get_barrier_semaphore()
    for r in range(1, nodes):
        pl.semaphore_signal(barrier, inc=1, device_id=(n ^ r, l), device_id_type=MESH)
    for mask in masks:
        pl.semaphore_signal(barrier, inc=1, device_id=(n, l ^ mask), device_id_type=MESH)

    loads = []
    stack = ((w0, w_in, 0), (w1, w_in, 1), (w3, w_in, 2), (w4, w_in, 3), (w2, w_out, 0), (w5, w_out, 1))
    for i, (w, buf, at) in enumerate(stack):
        load = pltpu.make_async_copy(w, buf.at[:, at * units : (at + 1) * units], load_sem.at[i])
        load.start()
        loads.append(load)

    pick, meta, absent, meta_rest = routing_plan(ids[...], gates[...], n, nodes, cap)
    pick_out[...] = pick.astype(BF16)
    pick_b, absent_b = pick.astype(BF16), absent.astype(BF16)

    def place(r, columns, values):
        if r == 0:
            rows[0, 0, :, columns] = values
        else:
            away[r - 1, :, columns] = values

    tile = width // 7
    for source, base in ((tok, 0), (grad, width)):
        for c in range(7):
            chosen = dot(pick_b, source[:, c * tile : (c + 1) * tile])
            for r in range(nodes):
                place(
                    r, pl.ds(base + c * tile, tile),
                    chosen[r * cap : (r + 1) * cap].astype(BF16),
                )
    for r in range(nodes):
        place(r, pl.ds(2 * width, LANES), meta[r * cap : (r + 1) * cap].astype(BF16))

    pl.semaphore_wait(barrier, nodes - 1 + bits)

    arrived = {}
    buffers = {"rows": (rows, width), "ext": (ext, piece)}

    def pass_on(name, k, p, columns):
        buf, _ = buffers[name]
        for b in range(2, bits):
            if p < 1 << b:
                q = p + (1 << b)
                arrived.setdefault((name, k, q), []).append((columns, remote(
                    buf.at[k, p, :, columns], buf.at[k, q, :, columns], (n, l ^ masks[b])
                )))

    def own(name, k):
        buf, _ = buffers[name]
        for b in range(2):
            arrived[name, k, 1 << b] = [(None, remote(
                buf.at[k, 0], buf.at[k, 1 << b], (n, l ^ masks[b])
            ))]
        pass_on(name, k, 0, slice(None))

    def forward(name, k):
        buf, split = buffers[name]
        ends = buf.shape[-1]
        parts = (pl.ds(0, split), pl.ds(split, ends - split))
        for p, over in ((1, 1), (2, 0)):
            for _, copy in arrived[name, k, p]:
                copy.wait_recv()
            columns = parts[p - 1]
            arrived.setdefault((name, k, 3), []).append((columns, remote(
                buf.at[k, p, :, columns], buf.at[k, 3, :, columns], (n, l ^ masks[over])
            )))
            pass_on(name, k, p, slice(None))

    def corner(name, k):
        for p in range(3, local_count // 2):
            for columns, copy in list(arrived[name, k, p]):
                copy.wait_recv()
                pass_on(name, k, p, columns)

    def complete(name, k):
        for p in range(local_count // 2, local_count):
            for _, copy in arrived[name, k, p]:
                copy.wait_recv()

    entering = {}
    own("rows", 0)
    for k in range(1, nodes):
        r = order[k]
        entering["rows", k] = pltpu.make_async_remote_copy(
            src_ref=away.at[r - 1], dst_ref=rows.at[k, 0],
            send_sem=cross_send.at[k - 1], recv_sem=cross_recv.at[k - 1],
            device_id=(n ^ r, l), device_id_type=MESH,
        )
    for k in range(1, nodes):
        entering["rows", k].start()

    for r in range(nodes):
        start = pl.multiple_of((n ^ r) * piece, LANES)
        these = absent_b[r * rest : (r + 1) * rest]
        values = [
            (pl.ds(0, piece), dot(these, tok[:, pl.ds(start, piece)])),
            (pl.ds(piece, piece), dot(these, grad[:, pl.ds(start, piece)])),
            (pl.ds(2 * piece, LANES), meta_rest[r * rest : (r + 1) * rest]),
        ]
        for columns, value in values:
            if r == 0:
                ext[0, 0, :, columns] = value.astype(BF16)
            else:
                mine[r - 1, :, columns] = value.astype(BF16)

    def cross_ext():
        for k in range(1, nodes):
            r = order[k]
            entering["ext", k] = remote(mine.at[r - 1], ext.at[k, 0], (n ^ r, l))

    def enter(name, k):
        entering[name, k].wait_recv()
        own(name, k)

    expert = l // (local_count // E_NODE)
    deep = width // 7
    block = local_count * cap

    def chunk(k0, m, columns):
        return rows[k0 : k0 + m, :, :, columns].reshape(m * block, -1)

    def ffn(g):
        k0, m = spans[g]
        total = m * block
        pre[0:total, :] = jnp.zeros((total, 6 * units), F32)

        def step(c, carry):
            at = pl.multiple_of(c * (width // 2), LANES)
            here = pl.ds(at, width // 2)
            pre[0:total, 0 : 4 * units] += dot(chunk(k0, m, here), w_in[here, :])
            left_g = chunk(k0, m, pl.ds(width + at, width // 2))
            pre[0:total, 4 * units :] += dot(left_g, w_out[here, :])
            return carry

        lax.fori_loop(0, 2, step, 0)
        table = chunk(k0, m, pl.ds(2 * width, LANES)).astype(F32)
        weight = jnp.where(expert == 0, table[:, 0:1], table[:, 1:2])
        is_shared = flag((iota((total, 1), 0) & (cap - 1)) < half)
        p, q, p_s, q_s, u, u_s = (pre[0:total, i * units : (i + 1) * units] for i in range(6))
        gg, gu, gh, product = ffn_backward(p, q, u, weight)
        sg, su, sh, _ = ffn_backward(p_s, q_s, u_s, is_shared)
        for i, value in enumerate((gg, gu, sg, su, gh)):
            grads[k0 * block : (k0 + m) * block, i * units : (i + 1) * units] = value
        score = jnp.sum(product, axis=1, keepdims=True)
        lanes = iota((total, LANES), 1)
        score = jnp.where(lanes == expert, score, 0.0)
        part[k0 : k0 + m, :, :, width:] = score.reshape(m, local_count, cap, LANES).astype(BF16)
        kept = m * seats
        shift, low = cap.bit_length() - 1, half.bit_length() - 1
        j, h = iota((kept, total), 0), iota((kept, total), 1)
        compact = flag(h == ((j >> low) << shift) + (j & (half - 1))).astype(BF16)
        for i, value in enumerate((sg, su, sh)):
            packs[0, k0 * seats : (k0 + m) * seats, i * units : (i + 1) * units] = dot(
                compact, value
            ).astype(BF16)

    turns = (dw_g, dw_u, dw_d, turned)

    def turn(i):
        loads[i].wait()
        eye = flag(iota((units, units), 0) == iota((units, units), 1)).astype(BF16)
        group = 4

        def step(c, carry):
            for sub in range(group):
                at = pl.ds(pl.multiple_of((c * group + sub) * units, LANES), units)
                turns[i][at, :] = contract_last(
                    eye, w_in[at, i * units : (i + 1) * units]
                ).astype(BF16)
            return carry

        lax.fori_loop(0, width // units // group, step, 0)

    def spread_dx(g, side):
        k0, m = spans[g]
        these = slice(k0 * block, (k0 + m) * block)
        group = 7
        count = width // 2 // units // group

        def step(c, carry):
            for sub in range(group):
                at = pl.ds(pl.multiple_of((c * group + sub) * units, LANES), units)
                total_dx = sum(
                    dot(grads[these, i * units : (i + 1) * units], turns[i][at, :])
                    for i in range(4)
                )
                part[k0 : k0 + m, :, :, at] = total_dx.reshape(m, local_count, cap, units).astype(
                    BF16
                )
            return carry

        lax.fori_loop(count * side, count * (side + 1), step, 0)

    def weight_grad(i, begin, end):
        base, first, outs = ((0, 0, (dw_g, dw_u)), (width, 4, (dw_d,)))[i]
        right = slice(first * units, (first + len(outs)) * units)
        size = deep

        def step(c, carry):
            at = pl.multiple_of(c * size, LANES)
            left = chunk(0, nodes, pl.ds(base + at, size))
            both = contract_first(left, grads[:, right]).astype(BF16)
            for o, out in enumerate(outs):
                out[pl.ds(at, size), :] = both[:, o * units : (o + 1) * units]
            return carry

        lax.fori_loop(begin, end, step, 0)

    def arrange(name):
        source, out, size = {"rows": (rows, near, cap), "ext": (ext, far, rest)}[name]
        shift, low = cap.bit_length() - 1, half.bit_length() - 1
        slots, columns = nodes * cap, nodes * seats
        seat = local_count.bit_length() - 1 + low
        h, j = iota((slots, columns), 0), iota((slots, columns), 1)
        widen = flag(
            ((h >> shift) == (j >> seat)) & ((h & (cap - 1)) == (j & (half - 1)))
        ).astype(BF16)
        block_of = (iota((1, columns), 1) & (seats - 1)) >> low
        height = local_count * size
        owner = jnp.zeros((height, 1), I32)
        for p in range(1, local_count):
            owner = owner + jnp.where(iota((height, 1), 0) >= p * size, 1, 0)
        meta = source.shape[-1] - LANES
        for k in range(nodes):
            table = jnp.concatenate([
                packs[order.index(order[k] ^ r), order.index(r) * seats : (order.index(r) + 1) * seats, :]
                for r in range(nodes)
            ], axis=0)
            perm = source[k, :, :, meta:].reshape(height, LANES)[:, PERM : PERM + slots]
            full = jnp.where(owner == block_of, dot(perm, widen), 0.0).astype(BF16)
            out[k * height : (k + 1) * height, :] = dot(full, table).astype(BF16)

    waits, packed = [], []

    def send_packs(g):
        k0, m = spans[g]
        these = pl.ds(k0 * seats, m * seats)
        for k in range(1, nodes):
            packed.append(remote(packs.at[0, these], packs.at[k, these], (n ^ order[k], l)))

    full = part.shape[-1]
    cut = width // 2
    sides = (pl.ds(0, cut), pl.ds(cut, full - cut))
    flight = {}
    upper = bits - 2
    last = upper + 1

    def moves(side, stage):
        if stage < upper:
            b = bits - 1 - stage
            return [(1 << b, 1 << b)], masks[b], 1 << b
        first = stage == upper
        if side == 0:
            return ([(1, 1), (3, 1)], masks[0], 1) if first else ([(2, 1)], masks[1], 2)
        return ([(2, 2)], masks[1], 2) if first else ([(1, 1)], masks[0], 1)

    def members(g):
        k0, m = spans[g]
        return range(k0 + m - 1, k0 - 1, -1)

    def launch(k, side, stage):
        blocks, mask, _ = moves(side, stage)
        flight[k, side, stage] = [
            (p, size, remote(
                part.at[k, pl.ds(p, size), :, sides[side]],
                land.at[k, pl.ds(p, size), :, sides[side]], (n, l ^ mask),
            ))
            for p, size in blocks
        ]

    def reduce_start(g, side):
        for k in members(g):
            launch(k, side, 0)

    def settle(k, side, stage):
        _, _, gap = moves(side, stage)
        columns = sides[side]
        for p, size, copy in flight[k, side, stage]:
            copy.wait_recv()

            def add(i, carry, p=p):
                there = land[k, p + i, :, columns].astype(F32)
                here = part[k, p + i - gap, :, columns].astype(F32)
                part[k, p + i - gap, :, columns] = (here + there).astype(BF16)
                return carry

            lax.fori_loop(0, size, add, 0)

    def go_home(k, side):
        columns = sides[side]
        if k == 0:
            back[0, :, columns] = part[0, 0, :, columns]
        else:
            waits.append(remote(
                part.at[k, 0, :, columns], back.at[order[k], :, columns], (n ^ order[k], l)
            ))

    def reduce_next(k, side, stage):
        settle(k, side, stage)
        if stage < last:
            launch(k, side, stage + 1)
        else:
            go_home(k, side)

    def reduce_both(g, stage):
        for k in members(g):
            for side in range(2):
                reduce_next(k, side, stage)

    half_way = spans[1][0]
    turn(0)
    turn(1)
    forward("rows", 0)
    own("ext", 0)
    turn(2)
    corner("rows", 0)
    for k in range(1, half_way):
        enter("rows", k)
    turn(3)
    for k in range(1, half_way):
        forward("rows", k)
    for k in range(half_way, nodes):
        enter("rows", k)
    for k in range(1, half_way):
        corner("rows", k)
    cross_ext()
    for load in loads[4:]:
        load.wait()
    for k in range(half_way):
        complete("rows", k)
    ffn(0)
    send_packs(0)
    for k in range(half_way, nodes - 1):
        forward("rows", k)
    spread_dx(0, 0)
    reduce_start(0, 0)
    forward("rows", nodes - 1)
    for k in range(half_way, nodes - 1):
        corner("rows", k)
    spread_dx(0, 1)
    reduce_start(0, 1)
    corner("rows", nodes - 1)
    reduce_both(0, 0)
    forward("ext", 0)
    for k in range(1, half_way):
        enter("ext", k)
    for k in range(half_way, nodes):
        complete("rows", k)
    ffn(1)
    send_packs(1)
    for side in range(2):
        spread_dx(1, side)
        reduce_start(1, side)
    todo = [(i, b, min(b + 1 + i, 7)) for i in range(2) for b in range(0, 7, 1 + i)]

    def fill(count):
        for _ in range(min(count, len(todo))):
            weight_grad(*todo.pop(0))

    reduce_both(0, 1)
    for side in range(2):
        for k in members(1):
            reduce_next(k, side, 0)
    for k in range(half_way, nodes):
        enter("ext", k)
    for stage in range(2, last + 1):
        fill(4)
        reduce_both(0, stage)
    for stage in range(1, last):
        for k in members(1):
            for side in range(2):
                reduce_next(k, side, stage)
            fill(2)
    for k in range(1, nodes):
        forward("ext", k)
    fill(1)
    for k in members(1):
        for side in range(2):
            reduce_next(k, side, last)
        fill(1)
    for k in range(nodes):
        corner("ext", k)
    fill(len(todo))
    for copy in packed:
        copy.wait_recv()
    arrange("rows")
    for k in range(nodes):
        complete("ext", k)
    arrange("ext")
    for copy in waits:
        copy.wait_recv()
    for k in range(1, nodes):
        entering["rows", k].wait_send()
    for copy in sends:
        copy.wait_send()


def room(scratch):
    held = sum(math.prod(dims) * jnp.dtype(kind).itemsize for dims, kind in scratch)
    return held + held // 32 + 3 * 2**20


def main_call(nodes, local_count, cap, tok, grad, ids, gates, weights):
    held, width = tok.shape
    units = weights[0].shape[1]
    rest, piece = held - cap, width // nodes
    most = max(m for _, m in spans_of(nodes)) * local_count * cap
    total = nodes * local_count * cap
    full, wide, narrow = width + LANES, 2 * width + LANES, 2 * piece + LANES
    vmem = pl.BlockSpec(memory_space=pltpu.VMEM)
    hbm = pl.BlockSpec(memory_space=pl.ANY)
    bits = local_count.bit_length() - 1
    gathers = 4 + sum(5 * 2 ** (b - 2) for b in range(2, bits))
    reduces = 2 * (bits - 2) + 5
    count = nodes * (2 * gathers + reduces) + (nodes - 1) * (3 + len(spans_of(nodes)))
    part = (nodes, local_count, cap, full)
    scratch = [
        ((nodes, total // 2, 3 * units), BF16),
        ((nodes - 1, cap, wide), BF16),
        ((nodes - 1, rest, narrow), BF16),
        ((width, 4 * units), BF16),
        ((width, 2 * units), BF16),
        ((width, units), BF16),
        (part, BF16),
        (part, BF16),
        ((most, 6 * units), F32),
        ((total, 5 * units), BF16),
    ]
    results = [
        (nodes, local_count, cap, wide),
        (nodes, local_count, rest, narrow),
        (total, 3 * units),
        (nodes * local_count * rest, 3 * units),
    ] + [(width, units)] * 3 + [(nodes, cap, full), (nodes * cap, held)]
    return pl.pallas_call(
        functools.partial(main_kernel, nodes, local_count, cap),
        out_shape=[pltpu.VMEM(dims, BF16) for dims in results],
        in_specs=[vmem] * 4 + [hbm] * 6,
        out_specs=[vmem] * 9,
        scratch_shapes=[pltpu.VMEM(*entry) for entry in scratch] + [
            pltpu.SemaphoreType.DMA((count,)),
            pltpu.SemaphoreType.DMA((count,)),
            pltpu.SemaphoreType.DMA((nodes - 1,)),
            pltpu.SemaphoreType.DMA((nodes - 1,)),
            pltpu.SemaphoreType.DMA((6,)),
        ],
        compiler_params=pltpu.CompilerParams(
            collective_id=0, has_side_effects=True, vmem_limit_bytes=room(scratch)
        ),
        name="exchange",
    )(tok, grad, ids, gates, *weights)


def finish_kernel(
    cap,
    rows, ext, near, far, dw_g, dw_u, dw_d, back, pick, ids,
    out_g, out_u, out_d, ds_g, ds_u, ds_d, dx, dgates,
    ds, sem,
):
    n = lax.axis_index("node")
    width, units = dw_g.shape
    piece = ds.shape[1]
    slots = pick.shape[0]
    copies = []

    def store(src, dst):
        copy = pltpu.make_async_copy(src, dst, sem.at[len(copies)])
        copy.start()
        copies.append(copy)

    for src, dst in ((dw_g, out_g), (dw_u, out_u), (dw_d, out_d)):
        store(src, dst)

    size = piece // 7
    for i, count in enumerate((2, 1)):
        cols = slice(2 * i * units, (2 * i + count) * units)

        def step(c, carry, i=i, cols=cols, count=count):
            at = pl.multiple_of(c * size, LANES)
            there = pl.multiple_of(i * width + n * piece + at, LANES)
            a = rows[:, :, :, pl.ds(there, size)].reshape(near.shape[0], size)
            b = ext[:, :, :, pl.ds(i * piece + at, size)].reshape(far.shape[0], size)
            value = contract_first(a, near[:, cols]) + contract_first(b, far[:, cols])
            for o in range(count):
                ds[2 * i + o, pl.ds(at, size), :] = value[
                    :, o * units : (o + 1) * units
                ].astype(BF16)
            return carry

        lax.fori_loop(0, 7, step, 0)
        for o in range(count):
            store(ds.at[2 * i + o], (ds_g, ds_u, ds_d)[2 * i + o])

    flat = back[...].reshape(slots, back.shape[-1])
    tile = width // 7
    for c in range(7):
        cols = slice(c * tile, (c + 1) * tile)
        dx[:, cols] = contract_first(pick[...], flat[:, cols]).astype(BF16)
    score = flat[:, width:].astype(F32)
    rel = (ids[...] >> 1) ^ n
    which = ids[...] & 1
    seen = pick[...].astype(F32)
    row_node = iota(seen.shape, 0) >> (cap.bit_length() - 1)
    total = jnp.zeros(dgates.shape, F32)
    for k in range(dgates.shape[0]):
        value = jnp.where(which[k : k + 1, :] == 0, score[:, 0:1], score[:, 1:2])
        value = jnp.where(row_node == rel[k : k + 1, :], seen * value, 0.0)
        value = jnp.sum(value, axis=0, keepdims=True)
        total = jnp.where(iota(dgates.shape, 0) == k, value, total)
    dgates[...] = total
    for copy in copies:
        copy.wait()


def finish_call(nodes, cap, values, ids):
    width, units = values[4].shape
    vmem = pl.BlockSpec(memory_space=pltpu.VMEM)
    hbm = pl.BlockSpec(memory_space=pl.ANY)
    shape = jax.ShapeDtypeStruct
    piece = width // nodes
    scratch = [((3, piece, units), BF16)]
    return pl.pallas_call(
        functools.partial(finish_kernel, cap),
        in_specs=[vmem] * 10,
        out_specs=[hbm] * 6 + [vmem] * 2,
        out_shape=[shape((width, units), BF16)] * 3 + [shape((piece, units), BF16)] * 3 + [
            shape((ids.shape[1], width), BF16), shape(ids.shape, F32),
        ],
        scratch_shapes=[pltpu.VMEM(*entry) for entry in scratch] + [
            pltpu.SemaphoreType.DMA((6,)),
        ],
        compiler_params=pltpu.CompilerParams(vmem_limit_bytes=room(scratch)),
        name="finish",
    )(*values, ids)


def local(tokens, grad_out, gates, expert_ids, w_gate, w_up, w_down, s_gate, s_up, s_down):
    held, width = tokens.shape
    nodes, locals_ = lax.axis_size("node"), lax.axis_size("local")
    cap = 2 * held // nodes
    weights = (w_gate[0], w_up[0], w_down[0], s_gate, s_up, s_down)
    ids = expert_ids.T
    values = main_call(nodes, locals_, cap, tokens, grad_out, ids, gates.T, weights)
    dw_g, dw_u, dw_d, ds_g, ds_u, ds_d, dx, dgates = finish_call(
        nodes, cap, values, ids
    )
    return (dx, dgates.T, dw_g[None], dw_u[None], dw_d[None], ds_g, ds_u, ds_d)


def solution(mesh):
    token = P(("node", "local"), None)
    routed = P("node", None, "local")
    shared = P(None, "local")
    shared_out = P("node", "local")
    return jax.shard_map(
        local,
        mesh=mesh,
        in_specs=(token,) * 4 + (routed,) * 3 + (shared,) * 3,
        out_specs=(token,) * 2 + (routed,) * 3 + (shared_out,) * 3,
        check_vma=False,
    )
```
